256 devices in a mesh: ctx: 64 (over z, y, core), kvh: 4 (over x).
Axes of the slice: x: 4, y: 4, z: 8, core: 2. Of those that a mesh axis runs over, the one named last changes fastest.
Arguments:
- queries: bfloat16 [32768, 3584], P('ctx', 'kvh'), may hold values from -384 to 384
- key_block: bfloat16 [32768, 512], P('ctx', 'kvh'), may hold values from -8 to 8
- value_block: bfloat16 [32768, 512], P('ctx', 'kvh'), may hold values from -6 to 6
- block_valid: int32 [64], replicated, may hold values from 2 to 512, as said below
- out_weight: bfloat16 [3584, 3584], P('kvh'), may hold values from -6 to 6
Outputs:
- projected: bfloat16 [32768, 3584], P(('ctx', 'kvh'))
The draws below stay inside these ranges and needn't reach their ends.
Inputs may be any that keep to these rules, and one draw needn't show every extreme that they name: `block_valid`: every entry but the last equals 512.
All inputs are finite; a program needn't handle non-finite values.
Results may differ from the reference program's by a relative error of at most 0.01.
Values may be sent and summed in bfloat16 or wider, within the bound.
A program may use at most 128 MiB of HBM per device.

```python
import jax
import jax.numpy as jnp
from jax import lax

D = 3584
HD = 128
GROUP = 7
KV_HEADS = 4
BLK = 512
QDIM = 3584
TOKENS = 32768
N_CTX = 64


def joint_draw(key):
    block_count = N_CTX
    query_key, keys_key = jax.random.split(jax.random.fold_in(key, 7), 2)
    query_all = jax.random.truncated_normal(query_key, -4.0, 4.0, (block_count, BLK, KV_HEADS, GROUP, HD), jnp.float32)
    key_all = jax.random.truncated_normal(keys_key, -4.0, 4.0, (block_count, BLK, KV_HEADS, HD), jnp.float32)
    return (query_all, key_all)


def draw_queries(key, part):
    query_all, key_all = joint_draw(key)
    return query_all.reshape(N_CTX * BLK, KV_HEADS * GROUP * HD).astype(jnp.bfloat16)


def draw_key_block(key, part):
    query_all, key_all = joint_draw(key)
    return key_all.reshape(N_CTX * BLK, KV_HEADS * HD).astype(jnp.bfloat16)


def draw_block_valid(key, part):
    last_count = jax.random.randint(jax.random.fold_in(key, 11), (), 2, BLK + 1, jnp.int32)
    return jnp.full((N_CTX,), BLK, jnp.int32).at[N_CTX - 1].set(last_count)


def block_levels(rng, shape, cuts, low, top_value):
    loudness = 1.0
    for axis_at, shards_of in cuts:
        heights = jax.random.uniform(jax.random.fold_in(jax.random.fold_in(rng, 6), axis_at), (shards_of,), jnp.float32, low / len(cuts), top_value / len(cuts))
        loudness = loudness * jnp.repeat(jnp.exp(heights), shape[axis_at] // shards_of).reshape((-1,) + (1,) * (len(shape) - 1 - axis_at))
    return loudness


def bell_draw(own_key, dims, spread, bound, cuts=(), kind=jnp.bfloat16):
    gain = block_levels(own_key, dims, cuts, -0.22, 0.18) if cuts else 1.0
    array = jax.random.normal(own_key, dims, jnp.float32) * spread * gain
    return jnp.minimum(jnp.maximum(array, -bound), bound).astype(kind)


def setup_inputs(seed: int = 0) -> dict:
    streams_of = jax.random.split(jax.random.key(seed), 6)
    return {
        "queries": draw_queries(jax.random.fold_in(streams_of[5], 71), 0),
        "key_block": draw_key_block(jax.random.fold_in(streams_of[5], 71), 0),
        "value_block": bell_draw(streams_of[2], (TOKENS, KV_HEADS * HD), 1.0, 6.0, ((0, 64), (1, 4))),
        "block_valid": draw_block_valid(jax.random.fold_in(streams_of[5], 71), 0),
        "out_weight": bell_draw(streams_of[4], (QDIM, D), (max(1, QDIM // (7 * BLK))) ** -0.5, 6.0, ((0, 4),)),
    }


def reference(queries, key_block, value_block, block_valid, out_weight):
    block_count = N_CTX
    offsets = [1 << level_id for level_id in range((block_count - 1).bit_length())]
    query_all = queries.reshape(block_count, BLK, KV_HEADS, GROUP, HD)
    key_all = key_block.reshape(block_count, BLK, KV_HEADS, HD)
    value_all = value_block.reshape(block_count, BLK, KV_HEADS, HD)
    position = jnp.arange(BLK, dtype=jnp.int32)
    score_scale = HD ** -0.5

    def attend(block_id):
        key_list = [lax.dynamic_index_in_dim(key_all, block_id, 0, keepdims=False)]
        value_list = [lax.dynamic_index_in_dim(value_all, block_id, 0, keepdims=False)]
        mask_list = [(position[None, :] <= position[:, None]) & (position[None, :] < block_valid[block_id])]
        for offset in offsets:
            source = jnp.maximum(block_id - offset, 0).astype(jnp.int32)
            key_list.append(lax.dynamic_index_in_dim(key_all, source, 0, keepdims=False))
            value_list.append(lax.dynamic_index_in_dim(value_all, source, 0, keepdims=False))
            usable = (block_id - offset >= 0) & (position < block_valid[source])
            mask_list.append(jnp.broadcast_to(usable[None, :], (BLK, BLK)))
        keys_cat = jnp.concatenate(key_list, axis=0)
        values_cat = jnp.concatenate(value_list, axis=0)
        allowed = jnp.concatenate(mask_list, axis=1)
        query_now = lax.dynamic_index_in_dim(query_all, block_id, 0, keepdims=False)
        scores = jnp.einsum("qhgd,khd->hgqk", query_now.astype(jnp.float32), keys_cat.astype(jnp.float32)) * score_scale
        scores = jnp.where(allowed, scores, -1e30)
        row_max = jnp.max(scores, axis=-1, keepdims=True)
        numerators = jnp.where(allowed, jnp.exp(scores - row_max), 0.0)
        row_total = jnp.sum(numerators, axis=-1)
        weights = lax.optimization_barrier(numerators.astype(jnp.bfloat16))
        mixture = jnp.einsum("hgqk,khd->hgqd", weights.astype(jnp.float32), values_cat.astype(jnp.float32))
        mixture = mixture / row_total[..., None]
        return jnp.transpose(mixture, (2, 0, 1, 3)).reshape(BLK, KV_HEADS * GROUP * HD).astype(jnp.bfloat16)

    attended = lax.map(attend, jnp.arange(block_count, dtype=jnp.int32)).reshape(block_count * BLK, KV_HEADS * GROUP * HD)
    slab_width = GROUP * HD
    summed = jnp.zeros((attended.shape[0], out_weight.shape[1]), jnp.float32)
    for head_id in range(KV_HEADS):
        partial_value = jnp.dot(attended[:, head_id * slab_width:(head_id + 1) * slab_width],
                          out_weight[head_id * slab_width:(head_id + 1) * slab_width],
                          preferred_element_type=jnp.float32).astype(jnp.bfloat16)
        summed = summed + lax.optimization_barrier(partial_value).astype(jnp.float32)
    return summed.astype(jnp.bfloat16)
```

```python
import contextlib
import math

import jax
import jax.numpy as jnp
from jax import lax
from jax.experimental import pallas as pl
from jax.experimental.pallas import tpu as pltpu
from jax.sharding import PartitionSpec as P

MESH = pl.DeviceIdType.MESH
TRACE = False
OWN, S1, S2, S4, S8, S16, S32, RELAY = range(8)
OFFSETS = {S1: 1, S2: 2, S4: 4, S8: 8, S16: 16, S32: 32}


def scope(name):
    return jax.named_scope(name) if TRACE else contextlib.nullcontext()


def kernel(
    valid_ref, q_hbm, k_hbm, v_hbm, w_hbm, o_hbm,
    q_s, kv, vt, w_s, acc, m_s, att, own_s, out_s,
    far_send, far_recv, near_send, near_recv,
    load_sem, w_sem, kv_send, kv_recv, fs_sem, fr_sem, ns_sem, nr_sem, out_sem,
):
    rows, qcols = q_hbm.shape
    hd = k_hbm.shape[1]
    heads = qcols // hd
    chunk = rows // 4
    pw = out_s.shape[2]
    np_ = out_s.shape[0]
    half = np_ // 2
    c = lax.axis_index("ctx")
    h = lax.axis_index("kvh")
    core = lax.rem(c, 2)
    y = lax.rem(c // 2, 4)
    z = c // 8

    def at(dz, dy):
        return lax.rem(z + 8 + dz, 8) * 8 + lax.rem(y + 4 + dy, 4) * 2 + core

    right, left = lax.rem(h + 1, 4), lax.rem(h + 3, 4)
    partner = c + 1 - 2 * core

    chunk_ids = [lax.rem(h + 2, 4), right, left, h]
    loads = []
    k_load = pltpu.make_async_copy(k_hbm, kv.at[OWN, 0], load_sem.at[0])
    v_load = pltpu.make_async_copy(v_hbm, kv.at[OWN, 1], load_sem.at[1])
    k_load.start()
    v_load.start()
    for i, cid in enumerate(chunk_ids):
        src = q_hbm.at[pl.ds(pl.multiple_of(cid * chunk, chunk), chunk), :]
        cp = pltpu.make_async_copy(src, q_s.at[pl.ds(i * chunk, chunk), :], load_sem.at[2 + i])
        cp.start()
        loads.append(cp)
    w_load = pltpu.make_async_copy(w_hbm, w_s, w_sem)
    w_load.start()

    barrier = pltpu.get_barrier_semaphore()
    senders = [
        (at(-1, 0), h), (at(1, 0), h), (at(-2, 0), h), (at(3, 0), h),
        (at(0, -1), h), (at(0, -2), h), (partner, h), (c, left), (c, right),
    ]
    with scope("entry"):
        for dev in senders:
            pl.semaphore_signal(barrier, inc=1, device_id=dev, device_id_type=MESH)
        pl.semaphore_wait(barrier, len(senders))

    def kv_copy(src_slot, dst_slot, part, dev):
        return pltpu.make_async_remote_copy(
            src_ref=kv.at[src_slot, part], dst_ref=kv.at[dst_slot, part],
            send_sem=kv_send.at[dst_slot, part], recv_sem=kv_recv.at[dst_slot, part],
            device_id=dev, device_id_type=MESH,
        )

    def arrived(slot, part):
        with scope(f"wait_{slot}_{part}"):
            kv_copy(OWN, slot, part, (c, h)).wait_recv()

    z_up, z_up2, z_down, z_down3 = (at(1, 0), h), (at(2, 0), h), (at(-1, 0), h), (at(-3, 0), h)
    y_up, y_up2 = (at(0, 1), h), (at(0, 2), h)
    other = (partner, h)

    k_load.wait()
    v_load.wait()
    kv_copy(OWN, S8, 0, z_up).start()
    kv_copy(OWN, RELAY, 1, z_down).start()
    kv_copy(OWN, S8, 1, z_up).start()

    @pl.when(y < 3)
    def _():
        kv_copy(OWN, S2, 0, y_up).start()
        kv_copy(OWN, S2, 1, y_up).start()

    @pl.when(y < 2)
    def _():
        kv_copy(OWN, S4, 0, y_up2).start()
        kv_copy(OWN, S4, 1, y_up2).start()

    @pl.when(core == 0)
    def _():
        kv_copy(OWN, S1, 0, other).start()
        kv_copy(OWN, S1, 1, other).start()

    scale = hd ** -0.5 * math.log2(math.e)
    blk_valid = valid_ref[c]
    ones_rows = vt.shape[0] - hd
    vt[pl.ds(hd, ones_rows), :] = jnp.ones((ones_rows, rows), vt.dtype)
    acc[...] = jnp.zeros_like(acc)
    m_s[...] = jnp.full_like(m_s, -1e30)

    def block_step(slot, pair, g, diag):
        q = q_s[pl.ds(pl.multiple_of(pair * 2 * chunk, 2 * chunk), 2 * chunk), g * hd:(g + 1) * hd]
        s = lax.dot_general(
            kv[slot, 0], q, (((1,), (1,)), ((), ())), preferred_element_type=jnp.float32
        )
        if diag:
            key_at = lax.broadcasted_iota(jnp.int32, s.shape, 0)
            col = lax.broadcasted_iota(jnp.int32, s.shape, 1)
            first = jnp.where(pair == 0, chunk_ids[0], chunk_ids[2])
            second = jnp.where(pair == 0, chunk_ids[1], chunk_ids[3])
            query_at = jnp.where(col < chunk, first * chunk + col, second * chunk + col - chunk)
            s = jnp.where((key_at <= query_at) & (key_at < blk_valid), s, -1e30)
        m_old = m_s[pair, g, 0:1, :]
        m_new = jnp.maximum(m_old, jnp.max(s, axis=0, keepdims=True))
        p = jnp.exp2((s - m_new) * scale).astype(jnp.bfloat16)
        alpha = jnp.exp2((m_old - m_new) * scale)
        pv = jnp.dot(vt[...], p, preferred_element_type=jnp.float32)
        acc[pair, g] = acc[pair, g] * alpha + pv
        m_s[pair, g] = jnp.broadcast_to(m_new, m_s.shape[2:])

    def set_vt(slot):
        vt[pl.ds(0, hd), :] = kv[slot, 1].T

    def block(slot, pair, diag=False):
        for g in range(heads):
            block_step(slot, pair, g, diag)

    def both(slot, diag=False):
        with scope(f"both_{slot}"):
            set_vt(slot)

            @pl.loop(0, 2)
            def _(pair):
                block(slot, pair, diag)

    with scope("blk_own"):
        for cp in loads:
            cp.wait()
        both(OWN, diag=True)

    for part in range(2):
        arrived(S8, part)
        kv_copy(S8, S16, part, z_up).start()

        @pl.when(y == 3)
        def _():
            kv_copy(S8, S2, part, y_up).start()

        @pl.when(y >= 2)
        def _():
            kv_copy(S8, S4, part, y_up2).start()

    arrived(RELAY, 1)
    kv_copy(RELAY, S32, 1, z_down3).start()

    @pl.when(c >= 8)
    def _():
        both(S8)

    for part in range(2):
        arrived(S2, part)

        @pl.when(core == 1)
        def _():
            kv_copy(S2, S1, part, other).start()

    @pl.when(c >= 2)
    def _():
        both(S2)

    arrived(S16, 0)
    kv_copy(S16, S32, 0, z_up2).start()

    for slot in (S1, S4, S16):
        arrived(slot, 1)
        if slot != S16:
            arrived(slot, 0)

        @pl.when(c >= OFFSETS[slot])
        def _():
            both(slot)

    arrived(S32, 0)
    arrived(S32, 1)

    @pl.when(c >= 32)
    def _():
        with scope("last_0"):
            set_vt(S32)
            block(S32, 0)

    def finish(pair):
        for g in range(heads):
            full = acc[pair, g]
            mix = full[:hd, :] / full[hd:hd + 1, :]
            att[pl.ds(pl.multiple_of(pair * 2 * chunk, 2 * chunk), 2 * chunk), g * hd:(g + 1) * hd] = (
                mix.T.astype(jnp.bfloat16)
            )

    def partial(i, piece):
        cols = pl.ds(pl.multiple_of(piece * pw, pw), pw)
        return jnp.dot(
            att[i * chunk:(i + 1) * chunk, :], w_s[:, cols], preferred_element_type=jnp.float32
        )

    def far_copy(side, j):
        piece = j if side == 0 else half + j
        return pltpu.make_async_remote_copy(
            src_ref=far_send.at[piece], dst_ref=far_recv.at[side, j],
            send_sem=fs_sem.at[side, j], recv_sem=fr_sem.at[side, j],
            device_id=(c, right if side == 0 else left), device_id_type=MESH,
        )

    def near_copy(side, piece):
        return pltpu.make_async_remote_copy(
            src_ref=near_send.at[side, piece], dst_ref=near_recv.at[side, piece],
            send_sem=ns_sem.at[side, piece], recv_sem=nr_sem.at[side, piece],
            device_id=(c, right if side == 0 else left), device_id_type=MESH,
        )

    with scope("finish_0"):
        finish(0)
        w_load.wait()

    with scope("far"):
        @pl.loop(0, half)
        def _(j):
            far_send[j] = partial(0, j).astype(jnp.bfloat16)
            far_copy(0, j).start()
            far_send[half + j] = partial(0, half + j).astype(jnp.bfloat16)
            far_copy(1, j).start()

    @pl.when(c >= 32)
    def _():
        with scope("last_1"):
            block(S32, 1)

    with scope("finish_1"):
        finish(1)

    with scope("near_plain"):
        @pl.loop(0, half)
        def _(j):
            near_send[0, half + j] = partial(1, half + j).astype(jnp.bfloat16)
            near_copy(0, half + j).start()
            near_send[1, j] = partial(2, j).astype(jnp.bfloat16)
            near_copy(1, j).start()

    with scope("own_part"):
        @pl.loop(0, np_)
        def _(j):
            own_s[j] = partial(3, j)

    with scope("near_sum"):
        @pl.loop(0, half)
        def _(j):
            mine = partial(1, j)
            far_copy(0, j).wait_recv()
            near_send[0, j] = (mine + far_recv[0, j].astype(jnp.float32)).astype(jnp.bfloat16)
            near_copy(0, j).start()
            mine = partial(2, half + j)
            far_copy(1, j).wait_recv()
            near_send[1, half + j] = (mine + far_recv[1, j].astype(jnp.float32)).astype(jnp.bfloat16)
            near_copy(1, half + j).start()

    def out_copy(piece):
        return pltpu.make_async_copy(
            out_s.at[piece], o_hbm.at[:, pl.ds(pl.multiple_of(piece * pw, pw), pw)], out_sem.at[piece]
        )

    def final(piece):
        near_copy(0, piece).wait_recv()
        near_copy(1, piece).wait_recv()
        out_s[piece] = (
            own_s[piece] + near_recv[0, piece].astype(jnp.float32) + near_recv[1, piece].astype(jnp.float32)
        ).astype(out_s.dtype)
        out_copy(piece).start()

    with scope("final"):
        @pl.loop(0, half)
        def _(j):
            final(j)
            final(half + j)

    for slot in (S2, S4, S1, S8, S16, S32):
        for part in range(2):
            kv_copy(OWN, slot, part, (c, h)).wait_send()
    kv_copy(OWN, RELAY, 1, (c, h)).wait_send()

    @pl.loop(0, half)
    def _(j):
        far_copy(0, j).wait_send()
        far_copy(1, j).wait_send()

    @pl.loop(0, np_)
    def _(j):
        near_copy(0, j).wait_send()
        near_copy(1, j).wait_send()
        out_copy(j).wait()


def per_device(queries, key_block, value_block, block_valid, out_weight):
    rows, qcols = queries.shape
    hd = key_block.shape[1]
    heads = qcols // hd
    d = out_weight.shape[1]
    chunk = rows // 4
    pw = 256
    np_ = d // pw
    half = np_ // 2
    bf16, f32 = jnp.bfloat16, jnp.float32
    any_spec = pl.BlockSpec(memory_space=pl.ANY)
    return pl.pallas_call(
        kernel,
        out_shape=jax.ShapeDtypeStruct((chunk, d), bf16),
        in_specs=[pl.BlockSpec(memory_space=pltpu.SMEM)] + [any_spec] * 4,
        out_specs=any_spec,
        scratch_shapes=[
            pltpu.VMEM((rows, qcols), bf16),
            pltpu.VMEM((8, 2, rows, hd), bf16),
            pltpu.VMEM((hd + 16, rows), bf16),
            pltpu.VMEM((qcols, d), bf16),
            pltpu.VMEM((2, heads, hd + 16, 2 * chunk), f32),
            pltpu.VMEM((2, heads, 8, 2 * chunk), f32),
            pltpu.VMEM((rows, qcols), bf16),
            pltpu.VMEM((np_, chunk, pw), f32),
            pltpu.VMEM((np_, chunk, pw), bf16),
            pltpu.VMEM((np_, chunk, pw), bf16),
            pltpu.VMEM((2, half, chunk, pw), bf16),
            pltpu.VMEM((2, np_, chunk, pw), bf16),
            pltpu.VMEM((2, np_, chunk, pw), bf16),
            pltpu.SemaphoreType.DMA((6,)),
            pltpu.SemaphoreType.DMA,
            pltpu.SemaphoreType.DMA((8, 2)),
            pltpu.SemaphoreType.DMA((8, 2)),
            pltpu.SemaphoreType.DMA((2, half)),
            pltpu.SemaphoreType.DMA((2, half)),
            pltpu.SemaphoreType.DMA((2, np_)),
            pltpu.SemaphoreType.DMA((2, np_)),
            pltpu.SemaphoreType.DMA((np_,)),
        ],
        compiler_params=pltpu.CompilerParams(
            collective_id=0, has_side_effects=True, vmem_limit_bytes=67_043_328
        ),
        name="attend_project",
    )(block_valid, queries, key_block, value_block, out_weight)


def solution(mesh):
    return jax.shard_map(
        per_device,
        mesh=mesh,
        in_specs=(P("ctx", "kvh"), P("ctx", "kvh"), P("ctx", "kvh"), P(), P("kvh", None)),
        out_specs=P(("ctx", "kvh"), None),
        check_vma=False,
    )
```

```python
import contextlib
import math

import jax
import jax.numpy as jnp
from jax import lax
from jax.experimental import pallas as pl
from jax.experimental.pallas import tpu as pltpu
from jax.sharding import PartitionSpec as P

MESH = pl.DeviceIdType.MESH
TRACE = False
OWN, S1, S2, S4, S8, S16, S32, RELAY, RELAY_Y = range(9)
OFFSETS = {S1: 1, S2: 2, S4: 4, S8: 8, S16: 16, S32: 32}


def scope(name):
    return jax.named_scope(name) if TRACE else contextlib.nullcontext()


def kernel(
    valid_ref, q_hbm, k_hbm, v_hbm, w_hbm, o_hbm,
    q_s, kv, vt, w_s, acc, m_s, s_s, p_s, alpha_s, att, own_s, out_s,
    far_send, far_recv, near_send, near_recv,
    load_sem, w_sem, kv_send, kv_recv, fs_sem, fr_sem, ns_sem, nr_sem, out_sem,
):
    rows, qcols = q_hbm.shape
    hd = k_hbm.shape[1]
    heads = qcols // hd
    chunk = rows // 4
    pw = out_s.shape[2]
    np_ = out_s.shape[0]
    half = np_ // 2
    c = lax.axis_index("ctx")
    h = lax.axis_index("kvh")
    core = lax.rem(c, 2)
    y = lax.rem(c // 2, 4)
    z = c // 8

    def at(dz, dy):
        return lax.rem(z + 8 + dz, 8) * 8 + lax.rem(y + 4 + dy, 4) * 2 + core

    right, left = lax.rem(h + 1, 4), lax.rem(h + 3, 4)
    partner = c + 1 - 2 * core

    chunk_ids = [lax.rem(h + 2, 4), right, left, h]
    loads = []
    k_load = pltpu.make_async_copy(k_hbm, kv.at[OWN, 0], load_sem.at[0])
    v_load = pltpu.make_async_copy(v_hbm, kv.at[OWN, 1], load_sem.at[1])
    k_load.start()
    v_load.start()
    for i, cid in enumerate(chunk_ids):
        src = q_hbm.at[pl.ds(pl.multiple_of(cid * chunk, chunk), chunk), :]
        cp = pltpu.make_async_copy(src, q_s.at[pl.ds(i * chunk, chunk), :], load_sem.at[2 + i])
        cp.start()
        loads.append(cp)
    w_load = pltpu.make_async_copy(w_hbm, w_s, w_sem)
    w_load.start()

    barrier = pltpu.get_barrier_semaphore()
    senders = [
        (at(-1, 0), h), (at(1, 0), h), (at(-2, 0), h), (at(3, 0), h),
        (at(0, -1), h), (at(0, 1), h), (partner, h), (c, left), (c, right),
    ]
    with scope("entry"):
        for dev in senders:
            pl.semaphore_signal(barrier, inc=1, device_id=dev, device_id_type=MESH)
        pl.semaphore_wait(barrier, len(senders))

    def kv_copy(src_slot, dst_slot, part, dev, sent_as=None):
        return pltpu.make_async_remote_copy(
            src_ref=kv.at[src_slot, part], dst_ref=kv.at[dst_slot, part],
            send_sem=kv_send.at[dst_slot if sent_as is None else sent_as, part],
            recv_sem=kv_recv.at[dst_slot, part],
            device_id=dev, device_id_type=MESH,
        )

    def arrived(slot, part):
        with scope(f"wait_{slot}_{part}"):
            kv_copy(OWN, slot, part, (c, h)).wait_recv()

    z_up, z_up2, z_down, z_down3 = (at(1, 0), h), (at(2, 0), h), (at(-1, 0), h), (at(-3, 0), h)
    y_up, y_down = (at(0, 1), h), (at(0, -1), h)
    other = (partner, h)

    k_load.wait()
    v_load.wait()
    kv_copy(OWN, S8, 0, z_up).start()
    kv_copy(OWN, RELAY, 1, z_down).start()
    kv_copy(OWN, S8, 1, z_up).start()

    @pl.when(y < 3)
    def _():
        kv_copy(OWN, S2, 0, y_up).start()
        kv_copy(OWN, S2, 1, y_up).start()

    @pl.when(core == 0)
    def _():
        kv_copy(OWN, S1, 0, other).start()
        kv_copy(OWN, S1, 1, other).start()

    scale = hd ** -0.5 * math.log2(math.e)
    blk_valid = valid_ref[c]
    ones_rows = vt.shape[1] - hd
    vt[:, hd:, :] = jnp.ones((vt.shape[0], ones_rows, rows), vt.dtype)
    acc[...] = jnp.zeros_like(acc)
    m_s[...] = jnp.full_like(m_s, -1e30)

    sub = rows // 2

    def tile_scores(slot, t, diag):
        pair, g = divmod(t, heads)
        q = q_s[pair * 2 * chunk:(pair + 1) * 2 * chunk, g * hd:(g + 1) * hd]
        m_old = m_s[t, 0:1, :]
        m_new = m_old
        for i in range(0, rows, sub):
            s = lax.dot_general(
                kv[slot, 0, i:i + sub, :], q, (((1,), (1,)), ((), ())), preferred_element_type=jnp.float32
            )
            if diag:
                key_at = i + lax.broadcasted_iota(jnp.int32, s.shape, 0)
                col = lax.broadcasted_iota(jnp.int32, s.shape, 1)
                first, second = chunk_ids[2 * pair], chunk_ids[2 * pair + 1]
                query_at = jnp.where(col < chunk, first * chunk + col, second * chunk + col - chunk)
                s = jnp.where((key_at <= query_at) & (key_at < blk_valid), s, -1e30)
            s_s[t % 2, i:i + sub] = s
            m_new = jnp.maximum(m_new, jnp.max(s, axis=0, keepdims=True))
        alpha_s[t % 3] = jnp.broadcast_to(jnp.exp2((m_old - m_new) * scale), alpha_s.shape[1:])
        m_s[t] = jnp.broadcast_to(m_new, m_s.shape[1:])

    def tile_weights(t):
        m = m_s[t, 0:1, :]
        for i in range(0, rows, sub):
            p_s[t % 2, i:i + sub] = jnp.exp2((s_s[t % 2, i:i + sub] - m) * scale).astype(p_s.dtype)

    def tile_mix(slot, t):
        pv = jnp.dot(vt[slot], p_s[t % 2], preferred_element_type=jnp.float32)
        acc[t] = acc[t] * alpha_s[t % 3, 0:1, :] + pv

    def tiles(slot, lo, hi, diag=False):
        tile_scores(slot, lo, diag)
        for t in range(lo, hi + 1):
            if t + 1 < hi:
                tile_scores(slot, t + 1, diag)
            if t < hi:
                tile_weights(t)
            if t > lo:
                tile_mix(slot, t - 1)

    def set_vt(slot):
        vt[slot, 0:hd, :] = kv[slot, 1].T

    def first_pair(slot):
        @pl.when(c >= OFFSETS[slot])
        def _():
            with scope(f"p0_{slot}"):
                set_vt(slot)
                tiles(slot, 0, heads)

    def second_pair(slot):
        @pl.when(c >= OFFSETS[slot])
        def _():
            with scope(f"p1_{slot}"):
                tiles(slot, heads, 2 * heads)

    with scope("blk_own"):
        for cp in loads:
            cp.wait()
        set_vt(OWN)
        tiles(OWN, 0, 2 * heads, True)

    for part in range(2):
        arrived(S8, part)
        kv_copy(S8, S16, part, z_up).start()

        @pl.when(y == 3)
        def _():
            kv_copy(S8, S2, part, y_up).start()

        @pl.when(y == 2)
        def _():
            kv_copy(S8, RELAY_Y, part, y_down).start()

    arrived(RELAY, 1)
    kv_copy(RELAY, S32, 1, z_down3).start()

    def pass_on_s2():
        for part in range(2):
            arrived(S2, part)

            @pl.when(core == 1)
            def _():
                kv_copy(S2, S1, part, other).start()

            @pl.when(y < 3)
            def _():
                kv_copy(S2, S4, part, y_up).start()

    pl.when(y > 0)(pass_on_s2)

    @pl.when(c >= OFFSETS[S8])
    def _():
        with scope("both_s8"):
            set_vt(S8)
            tiles(S8, 0, 2 * heads)

    arrived(S16, 0)
    kv_copy(S16, S32, 0, z_up2).start()
    pl.when(y == 0)(pass_on_s2)

    @pl.when(y == 1)
    def _():
        for part in range(2):
            arrived(RELAY_Y, part)
            kv_copy(RELAY_Y, S4, part, y_down, sent_as=RELAY_Y).start()

    first_pair(S2)
    for slot in (S1, S16):
        arrived(slot, 1)
        if slot != S16:
            arrived(slot, 0)
        first_pair(slot)

    @pl.when(y > 0)
    def _():
        second_pair(S2)

    for slot in (S4, S32):
        arrived(slot, 0)
        arrived(slot, 1)
        first_pair(slot)

    def finish(pair):
        for g in range(heads):
            full = acc[pair * heads + g]
            mix = full[:hd, :] / full[hd:hd + 1, :]
            att[pair * 2 * chunk:(pair + 1) * 2 * chunk, g * hd:(g + 1) * hd] = mix.T.astype(jnp.bfloat16)

    def partial(i, piece):
        cols = pl.ds(piece * pw if isinstance(piece, int) else pl.multiple_of(piece * pw, pw), pw)
        return jnp.dot(
            att[i * chunk:(i + 1) * chunk, :], w_s[:, cols], preferred_element_type=jnp.float32
        )

    def far_copy(side, j):
        piece = j if side == 0 else half + j
        return pltpu.make_async_remote_copy(
            src_ref=far_send.at[piece], dst_ref=far_recv.at[side, j],
            send_sem=fs_sem.at[side, j], recv_sem=fr_sem.at[side, j],
            device_id=(c, right if side == 0 else left), device_id_type=MESH,
        )

    def near_copy(side, piece):
        return pltpu.make_async_remote_copy(
            src_ref=near_send.at[side, piece], dst_ref=near_recv.at[side, piece],
            send_sem=ns_sem.at[side, piece], recv_sem=nr_sem.at[side, piece],
            device_id=(c, right if side == 0 else left), device_id_type=MESH,
        )

    with scope("finish_0"):
        finish(0)
        w_load.wait()

    bf16 = jnp.bfloat16

    with scope("far"):

        @pl.loop(0, half)
        def _(j):
            low, high = partial(0, j), partial(0, half + j)
            far_send[j] = low.astype(bf16)
            far_send[half + j] = high.astype(bf16)
            far_copy(0, j).start()
            far_copy(1, j).start()

    def plain(side, pieces):
        for at_piece in range(0, len(pieces), 2):
            group = pieces[at_piece:at_piece + 2]
            parts = [partial(1 + side, piece) for piece in group]
            for piece, value in zip(group, parts):
                near_send[side, piece] = value.astype(bf16)
            for piece in group:
                near_copy(side, piece).start()

    with scope("plain_right"):
        plain(0, list(range(half, np_)))

    @pl.when(y == 0)
    def _():
        second_pair(S2)

    for slot in (S1, S16, S4, S32):
        second_pair(slot)

    with scope("finish_1"):
        finish(1)

    with scope("plain_left"):
        plain(1, list(range(half)))

    with scope("near_sum"):

        @pl.loop(0, half)
        def _(j):
            low, high = partial(1, j), partial(2, half + j)
            far_copy(0, j).wait_recv()
            near_send[0, j] = (low + far_recv[0, j].astype(jnp.float32)).astype(bf16)
            near_copy(0, j).start()
            far_copy(1, j).wait_recv()
            near_send[1, half + j] = (high + far_recv[1, j].astype(jnp.float32)).astype(bf16)
            near_copy(1, half + j).start()

    with scope("own_part"):

        @pl.loop(0, half)
        def _(j):
            low, high = partial(3, j), partial(3, half + j)
            own_s[j] = low
            own_s[half + j] = high

    def out_copy(piece):
        return pltpu.make_async_copy(
            out_s.at[piece], o_hbm.at[:, pl.ds(pl.multiple_of(piece * pw, pw), pw)], out_sem.at[piece]
        )

    def final(piece):
        near_copy(0, piece).wait_recv()
        near_copy(1, piece).wait_recv()
        out_s[piece] = (
            own_s[piece] + near_recv[0, piece].astype(jnp.float32) + near_recv[1, piece].astype(jnp.float32)
        ).astype(out_s.dtype)
        out_copy(piece).start()

    with scope("final"):
        @pl.loop(0, half)
        def _(j):
            final(j)
            final(half + j)

    for part in range(2):
        for slot in (S2, S1, S8, S16, S32):
            kv_copy(OWN, slot, part, (c, h)).wait_send()

        @pl.when(y < 3)
        def _():
            kv_copy(OWN, S4, part, (c, h)).wait_send()

        @pl.when((y == 1) | (y == 2))
        def _():
            kv_copy(OWN, RELAY_Y, part, (c, h)).wait_send()
    kv_copy(OWN, RELAY, 1, (c, h)).wait_send()

    @pl.loop(0, half)
    def _(j):
        far_copy(0, j).wait_send()
        far_copy(1, j).wait_send()

    @pl.loop(0, np_)
    def _(j):
        near_copy(0, j).wait_send()
        near_copy(1, j).wait_send()
        out_copy(j).wait()


def per_device(queries, key_block, value_block, block_valid, out_weight):
    rows, qcols = queries.shape
    hd = key_block.shape[1]
    heads = qcols // hd
    d = out_weight.shape[1]
    chunk = rows // 4
    pw = 256
    np_ = d // pw
    half = np_ // 2
    bf16, f32 = jnp.bfloat16, jnp.float32
    any_spec = pl.BlockSpec(memory_space=pl.ANY)
    return pl.pallas_call(
        kernel,
        out_shape=jax.ShapeDtypeStruct((chunk, d), bf16),
        in_specs=[pl.BlockSpec(memory_space=pltpu.SMEM)] + [any_spec] * 4,
        out_specs=any_spec,
        scratch_shapes=[
            pltpu.VMEM((rows, qcols), bf16),
            pltpu.VMEM((9, 2, rows, hd), bf16),
            pltpu.VMEM((7, hd + 16, rows), bf16),
            pltpu.VMEM((qcols, d), bf16),
            pltpu.VMEM((2 * heads, hd + 16, 2 * chunk), f32),
            pltpu.VMEM((2 * heads, 8, 2 * chunk), f32),
            pltpu.VMEM((2, rows, 2 * chunk), f32),
            pltpu.VMEM((2, rows, 2 * chunk), bf16),
            pltpu.VMEM((3, 8, 2 * chunk), f32),
            pltpu.VMEM((rows, qcols), bf16),
            pltpu.VMEM((np_, chunk, pw), f32),
            pltpu.VMEM((np_, chunk, pw), bf16),
            pltpu.VMEM((np_, chunk, pw), bf16),
            pltpu.VMEM((2, half, chunk, pw), bf16),
            pltpu.VMEM((2, np_, chunk, pw), bf16),
            pltpu.VMEM((2, np_, chunk, pw), bf16),
            pltpu.SemaphoreType.DMA((6,)),
            pltpu.SemaphoreType.DMA,
            pltpu.SemaphoreType.DMA((9, 2)),
            pltpu.SemaphoreType.DMA((9, 2)),
            pltpu.SemaphoreType.DMA((2, half)),
            pltpu.SemaphoreType.DMA((2, half)),
            pltpu.SemaphoreType.DMA((2, np_)),
            pltpu.SemaphoreType.DMA((2, np_)),
            pltpu.SemaphoreType.DMA((np_,)),
        ],
        compiler_params=pltpu.CompilerParams(
            collective_id=0, has_side_effects=True, vmem_limit_bytes=67_043_328
        ),
        name="attend_project",
    )(block_valid, queries, key_block, value_block, out_weight)


def solution(mesh):
    return jax.shard_map(
        per_device,
        mesh=mesh,
        in_specs=(P("ctx", "kvh"), P("ctx", "kvh"), P("ctx", "kvh"), P(), P("kvh", None)),
        out_specs=P(("ctx", "kvh"), None),
        check_vma=False,
    )
```

```python
import contextlib
import math

import jax
import jax.numpy as jnp
from jax import lax
from jax.experimental import pallas as pl
from jax.experimental.pallas import tpu as pltpu
from jax.sharding import PartitionSpec as P

MESH = pl.DeviceIdType.MESH
TRACE = False
OWN, S1, S2, S4, S8, S16, S32, RELAY, RELAY_Y = range(9)
OFFSETS = {S1: 1, S2: 2, S4: 4, S8: 8, S16: 16, S32: 32}


def scope(name):
    return jax.named_scope(name) if TRACE else contextlib.nullcontext()


def kernel(
    valid_ref, q_hbm, k_hbm, v_hbm, w_hbm, o_ref,
    q_s, kv, vt, w_s, acc, m_s, s_s, p_s, alpha_s, att, own_s,
    far_send, far_recv, near_send, near_recv,
    load_sem, w_sem, kv_send, kv_recv, cut_send, cut_recv, fs_sem, fr_sem, ns_sem, nr_sem,
):
    rows, qcols = q_hbm.shape
    hd = k_hbm.shape[1]
    heads = qcols // hd
    chunk = rows // 4
    pw = own_s.shape[2]
    np_ = own_s.shape[0]
    half = np_ // 2
    c = lax.axis_index("ctx")
    h = lax.axis_index("kvh")
    core = lax.rem(c, 2)
    y = lax.rem(c // 2, 4)
    z = c // 8

    def at(dz, dy):
        return lax.rem(z + 8 + dz, 8) * 8 + lax.rem(y + 4 + dy, 4) * 2 + core

    right, left = lax.rem(h + 1, 4), lax.rem(h + 3, 4)
    partner = c + 1 - 2 * core

    chunk_ids = [lax.rem(h + 2, 4), right, left, h]
    loads = []
    k_load = pltpu.make_async_copy(k_hbm, kv.at[OWN, 0], load_sem.at[0])
    v_load = pltpu.make_async_copy(v_hbm, kv.at[OWN, 1], load_sem.at[1])
    k_load.start()
    v_load.start()
    for i, cid in enumerate(chunk_ids):
        src = q_hbm.at[pl.ds(pl.multiple_of(cid * chunk, chunk), chunk), :]
        cp = pltpu.make_async_copy(src, q_s.at[pl.ds(i * chunk, chunk), :], load_sem.at[2 + i])
        cp.start()
        loads.append(cp)
    w_load = pltpu.make_async_copy(w_hbm, w_s, w_sem)
    w_load.start()

    barrier = pltpu.get_barrier_semaphore()
    senders = [
        (at(-1, 0), h), (at(1, 0), h), (at(-2, 0), h), (at(3, 0), h),
        (at(0, -1), h), (at(0, 1), h), (partner, h), (c, left), (c, right),
    ]
    with scope("entry"):
        for dev in senders:
            pl.semaphore_signal(barrier, inc=1, device_id=dev, device_id_type=MESH)
        pl.semaphore_wait(barrier, len(senders))

    def kv_copy(src_slot, dst_slot, part, dev, sent_as=None):
        return pltpu.make_async_remote_copy(
            src_ref=kv.at[src_slot, part], dst_ref=kv.at[dst_slot, part],
            send_sem=kv_send.at[dst_slot if sent_as is None else sent_as, part],
            recv_sem=kv_recv.at[dst_slot, part],
            device_id=dev, device_id_type=MESH,
        )

    def arrived(slot, part):
        with scope(f"wait_{slot}_{part}"):
            kv_copy(OWN, slot, part, (c, h)).wait_recv()

    cut = rows * 3 // 4

    def cut_copy(src_slot, dst_slot, dev, low):
        part_rows = pl.ds(0, cut) if low else pl.ds(cut, rows - cut)
        sem = 0 if low else 1 if dst_slot == RELAY else 2
        return pltpu.make_async_remote_copy(
            src_ref=kv.at[src_slot, 0, part_rows], dst_ref=kv.at[dst_slot, 0, part_rows],
            send_sem=cut_send.at[sem], recv_sem=cut_recv.at[sem],
            device_id=dev, device_id_type=MESH,
        )

    z_up, z_up2, z_down, z_down3 = (at(1, 0), h), (at(2, 0), h), (at(-1, 0), h), (at(-3, 0), h)
    y_up, y_down = (at(0, 1), h), (at(0, -1), h)
    other = (partner, h)

    k_load.wait()
    v_load.wait()
    kv_copy(OWN, S8, 0, z_up).start()
    kv_copy(OWN, RELAY, 1, z_down).start()
    cut_copy(OWN, RELAY, z_down, False).start()
    kv_copy(OWN, S8, 1, z_up).start()

    @pl.when(y < 3)
    def _():
        kv_copy(OWN, S2, 0, y_up).start()
        kv_copy(OWN, S2, 1, y_up).start()

    @pl.when(core == 0)
    def _():
        kv_copy(OWN, S1, 0, other).start()
        kv_copy(OWN, S1, 1, other).start()

    scale = hd ** -0.5 * math.log2(math.e)
    blk_valid = valid_ref[c]
    ones_rows = vt.shape[1] - hd
    vt[:, hd:, :] = jnp.ones((vt.shape[0], ones_rows, rows), vt.dtype)
    acc[...] = jnp.zeros_like(acc)
    m_s[...] = jnp.full_like(m_s, -1e30)

    sub = rows // 2

    def tile_scores(slot, t, diag):
        pair, g = divmod(t, heads)
        q = q_s[pair * 2 * chunk:(pair + 1) * 2 * chunk, g * hd:(g + 1) * hd]
        m_old = m_s[t, 0:1, :]
        m_new = m_old
        for i in range(0, rows, sub):
            s = lax.dot_general(
                kv[slot, 0, i:i + sub, :], q, (((1,), (1,)), ((), ())), preferred_element_type=jnp.float32
            )
            if diag:
                key_at = i + lax.broadcasted_iota(jnp.int32, s.shape, 0)
                col = lax.broadcasted_iota(jnp.int32, s.shape, 1)
                first, second = chunk_ids[2 * pair], chunk_ids[2 * pair + 1]
                query_at = jnp.where(col < chunk, first * chunk + col, second * chunk + col - chunk)
                s = jnp.where((key_at <= query_at) & (key_at < blk_valid), s, -1e30)
            s_s[t % 2, i:i + sub] = s
            m_new = jnp.maximum(m_new, jnp.max(s, axis=0, keepdims=True))
        alpha_s[t % 3] = jnp.broadcast_to(jnp.exp2((m_old - m_new) * scale), alpha_s.shape[1:])
        m_s[t] = jnp.broadcast_to(m_new, m_s.shape[1:])

    def tile_weights(t):
        m = m_s[t, 0:1, :]
        for i in range(0, rows, sub):
            p_s[t % 2, i:i + sub] = jnp.exp2((s_s[t % 2, i:i + sub] - m) * scale).astype(p_s.dtype)

    def tile_mix(slot, t):
        pv = jnp.dot(vt[slot], p_s[t % 2], preferred_element_type=jnp.float32)
        acc[t] = acc[t] * alpha_s[t % 3, 0:1, :] + pv

    def tiles(slot, lo, hi, diag=False):
        tile_scores(slot, lo, diag)
        for t in range(lo, hi + 1):
            if t + 1 < hi:
                tile_scores(slot, t + 1, diag)
            if t < hi:
                tile_weights(t)
            if t > lo:
                tile_mix(slot, t - 1)

    def set_vt(slot):
        vt[slot, 0:hd, :] = kv[slot, 1].T

    def first_pair(slot):
        @pl.when(c >= OFFSETS[slot])
        def _():
            with scope(f"p0_{slot}"):
                set_vt(slot)
                tiles(slot, 0, heads)

    def second_pair(slot):
        @pl.when(c >= OFFSETS[slot])
        def _():
            with scope(f"p1_{slot}"):
                tiles(slot, heads, 2 * heads)

    with scope("blk_own"):
        for cp in loads:
            cp.wait()
        set_vt(OWN)
        tiles(OWN, 0, 2 * heads, True)

    @pl.when(core == 1)
    def _():
        arrived(S1, 0)
        arrived(S1, 1)
        first_pair(S1)

    def pass_on_s8(part):
        arrived(S8, part)
        kv_copy(S8, S16, part, z_up).start()

        @pl.when(y == 3)
        def _():
            kv_copy(S8, S2, part, y_up).start()

        @pl.when(y == 2)
        def _():
            kv_copy(S8, RELAY_Y, part, y_down).start()

    pass_on_s8(0)
    arrived(RELAY, 1)
    kv_copy(RELAY, S32, 1, z_down3).start()
    cut_copy(OWN, RELAY, (c, h), False).wait_recv()
    cut_copy(RELAY, S32, z_down3, False).start()

    @pl.when(core == 1)
    def _():
        second_pair(S1)

    pass_on_s8(1)

    def pass_on_s2():
        for part in range(2):
            arrived(S2, part)

            @pl.when(core == 1)
            def _():
                kv_copy(S2, S1, part, other).start()

            @pl.when(y < 3)
            def _():
                kv_copy(S2, S4, part, y_up).start()

    pl.when(y > 0)(pass_on_s2)

    @pl.when(c >= OFFSETS[S8])
    def _():
        with scope("both_s8"):
            set_vt(S8)
            tiles(S8, 0, 2 * heads)

    arrived(S16, 0)
    cut_copy(S16, S32, z_up2, True).start()
    pl.when(y == 0)(pass_on_s2)

    @pl.when(y == 1)
    def _():
        for part in range(2):
            arrived(RELAY_Y, part)
            kv_copy(RELAY_Y, S4, part, y_down, sent_as=RELAY_Y).start()

    first_pair(S2)

    @pl.when(core == 0)
    def _():
        arrived(S1, 0)
        arrived(S1, 1)
        first_pair(S1)

    arrived(S16, 1)
    first_pair(S16)
    early = (core == 1) & (y > 0)

    @pl.when(early)
    def _():
        second_pair(S2)

    arrived(S4, 0)
    arrived(S4, 1)
    first_pair(S4)
    cut_copy(OWN, S32, (c, h), True).wait_recv()
    cut_copy(OWN, S32, (c, h), False).wait_recv()
    arrived(S32, 1)
    first_pair(S32)

    def finish(pair):
        for g in range(heads):
            full = acc[pair * heads + g]
            mix = full[:hd, :] / full[hd:hd + 1, :]
            att[pair * 2 * chunk:(pair + 1) * 2 * chunk, g * hd:(g + 1) * hd] = mix.T.astype(jnp.bfloat16)

    def partial(i, piece):
        cols = pl.ds(piece * pw if isinstance(piece, int) else pl.multiple_of(piece * pw, pw), pw)
        return jnp.dot(
            att[i * chunk:(i + 1) * chunk, :], w_s[:, cols], preferred_element_type=jnp.float32
        )

    def far_copy(side, j):
        piece = j if side == 0 else half + j
        return pltpu.make_async_remote_copy(
            src_ref=far_send.at[piece], dst_ref=far_recv.at[side, j],
            send_sem=fs_sem.at[side, j], recv_sem=fr_sem.at[side, j],
            device_id=(c, right if side == 0 else left), device_id_type=MESH,
        )

    def near_copy(side, piece):
        return pltpu.make_async_remote_copy(
            src_ref=near_send.at[side, piece], dst_ref=near_recv.at[side, piece],
            send_sem=ns_sem.at[side, piece], recv_sem=nr_sem.at[side, piece],
            device_id=(c, right if side == 0 else left), device_id_type=MESH,
        )

    with scope("finish_0"):
        finish(0)
        w_load.wait()

    bf16 = jnp.bfloat16

    with scope("far"):

        @pl.loop(0, half)
        def _(j):
            low, high = partial(0, j), partial(0, half + j)
            far_send[j] = low.astype(bf16)
            far_send[half + j] = high.astype(bf16)
            far_copy(0, j).start()
            far_copy(1, j).start()

    def plain(side, pieces):
        for at_piece in range(0, len(pieces), 2):
            group = pieces[at_piece:at_piece + 2]
            parts = [partial(1 + side, piece) for piece in group]
            for piece, value in zip(group, parts):
                near_send[side, piece] = value.astype(bf16)
            for piece in group:
                near_copy(side, piece).start()

    with scope("plain_right"):
        plain(0, list(range(half, np_)))

    @pl.when(jnp.logical_not(early))
    def _():
        second_pair(S2)

    @pl.when(core == 0)
    def _():
        second_pair(S1)

    for slot in (S16, S4, S32):
        second_pair(slot)

    with scope("finish_1"):
        finish(1)

    with scope("plain_left"):
        plain(1, list(range(half)))

    with scope("near_sum"):

        @pl.loop(0, half)
        def _(j):
            low, high = partial(1, j), partial(2, half + j)
            far_copy(0, j).wait_recv()
            near_send[0, j] = (low + far_recv[0, j].astype(jnp.float32)).astype(bf16)
            near_copy(0, j).start()
            far_copy(1, j).wait_recv()
            near_send[1, half + j] = (high + far_recv[1, j].astype(jnp.float32)).astype(bf16)
            near_copy(1, half + j).start()

    with scope("own_part"):

        @pl.loop(0, half)
        def _(j):
            low, high = partial(3, j), partial(3, half + j)
            own_s[j] = low
            own_s[half + j] = high

    def final(piece):
        near_copy(0, piece).wait_recv()
        near_copy(1, piece).wait_recv()
        o_ref[:, pl.ds(pl.multiple_of(piece * pw, pw), pw)] = (
            own_s[piece] + near_recv[0, piece].astype(jnp.float32) + near_recv[1, piece].astype(jnp.float32)
        ).astype(o_ref.dtype)

    with scope("final"):
        @pl.loop(0, half)
        def _(j):
            final(j)
            final(half + j)

    for part in range(2):
        for slot in (S2, S1, S8, S16):
            kv_copy(OWN, slot, part, (c, h)).wait_send()

        @pl.when(y < 3)
        def _():
            kv_copy(OWN, S4, part, (c, h)).wait_send()

        @pl.when((y == 1) | (y == 2))
        def _():
            kv_copy(OWN, RELAY_Y, part, (c, h)).wait_send()
    kv_copy(OWN, RELAY, 1, (c, h)).wait_send()
    kv_copy(OWN, S32, 1, (c, h)).wait_send()
    cut_copy(OWN, S32, (c, h), True).wait_send()
    cut_copy(OWN, RELAY, (c, h), False).wait_send()
    cut_copy(OWN, S32, (c, h), False).wait_send()

    @pl.loop(0, half)
    def _(j):
        far_copy(0, j).wait_send()
        far_copy(1, j).wait_send()

    @pl.loop(0, np_)
    def _(j):
        near_copy(0, j).wait_send()
        near_copy(1, j).wait_send()


def per_device(queries, key_block, value_block, block_valid, out_weight):
    rows, qcols = queries.shape
    hd = key_block.shape[1]
    heads = qcols // hd
    d = out_weight.shape[1]
    chunk = rows // 4
    pw = 256
    np_ = d // pw
    half = np_ // 2
    bf16, f32 = jnp.bfloat16, jnp.float32
    any_spec = pl.BlockSpec(memory_space=pl.ANY)
    return pl.pallas_call(
        kernel,
        out_shape=pltpu.VMEM((chunk, d), bf16),
        in_specs=[pl.BlockSpec(memory_space=pltpu.SMEM)] + [any_spec] * 4,
        out_specs=pl.BlockSpec(memory_space=pltpu.VMEM),
        scratch_shapes=[
            pltpu.VMEM((rows, qcols), bf16),
            pltpu.VMEM((9, 2, rows, hd), bf16),
            pltpu.VMEM((7, hd + 16, rows), bf16),
            pltpu.VMEM((qcols, d), bf16),
            pltpu.VMEM((2 * heads, hd + 16, 2 * chunk), f32),
            pltpu.VMEM((2 * heads, 8, 2 * chunk), f32),
            pltpu.VMEM((2, rows, 2 * chunk), f32),
            pltpu.VMEM((2, rows, 2 * chunk), bf16),
            pltpu.VMEM((3, 8, 2 * chunk), f32),
            pltpu.VMEM((rows, qcols), bf16),
            pltpu.VMEM((np_, chunk, pw), f32),
            pltpu.VMEM((np_, chunk, pw), bf16),
            pltpu.VMEM((2, half, chunk, pw), bf16),
            pltpu.VMEM((2, np_, chunk, pw), bf16),
            pltpu.VMEM((2, np_, chunk, pw), bf16),
            pltpu.SemaphoreType.DMA((6,)),
            pltpu.SemaphoreType.DMA,
            pltpu.SemaphoreType.DMA((9, 2)),
            pltpu.SemaphoreType.DMA((9, 2)),
            pltpu.SemaphoreType.DMA((3,)),
            pltpu.SemaphoreType.DMA((3,)),
            pltpu.SemaphoreType.DMA((2, half)),
            pltpu.SemaphoreType.DMA((2, half)),
            pltpu.SemaphoreType.DMA((2, np_)),
            pltpu.SemaphoreType.DMA((2, np_)),
        ],
        compiler_params=pltpu.CompilerParams(
            collective_id=0, has_side_effects=True, vmem_limit_bytes=65_900_000
        ),
        name="attend_project",
    )(block_valid, queries, key_block, value_block, out_weight)


def solution(mesh):
    return jax.shard_map(
        per_device,
        mesh=mesh,
        in_specs=(P("ctx", "kvh"), P("ctx", "kvh"), P("ctx", "kvh"), P(), P("kvh", None)),
        out_specs=P(("ctx", "kvh"), None),
        check_vma=False,
    )
```

```python
import contextlib
import math

import jax
import jax.numpy as jnp
from jax import lax
from jax.experimental import pallas as pl
from jax.experimental.pallas import tpu as pltpu
from jax.sharding import PartitionSpec as P

MESH = pl.DeviceIdType.MESH
TRACE = False
OWN, S1, S2, S4, S8, S16, S32, RELAY, RELAY_Y = range(9)
OFFSETS = {S1: 1, S2: 2, S4: 4, S8: 8, S16: 16, S32: 32}


def scope(name):
    return jax.named_scope(name) if TRACE else contextlib.nullcontext()


def kernel(
    valid_ref, q_hbm, k_hbm, v_hbm, w_hbm, o_ref,
    q_s, kv, vt, w_s, acc, m_s, s_s, p_s, alpha_s, att, own_s,
    far_send, far_recv, near_send, near_recv,
    load_sem, w_sem, kv_send, kv_recv, cut_send, cut_recv, fs_sem, fr_sem, ns_sem, nr_sem,
):
    rows, qcols = q_hbm.shape
    hd = k_hbm.shape[1]
    heads = qcols // hd
    chunk = rows // 4
    pw = own_s.shape[2]
    np_ = own_s.shape[0]
    half = np_ // 2
    c = lax.axis_index("ctx")
    h = lax.axis_index("kvh")
    core = lax.rem(c, 2)
    y = lax.rem(c // 2, 4)
    z = c // 8

    def at(dz, dy):
        return lax.rem(z + 8 + dz, 8) * 8 + lax.rem(y + 4 + dy, 4) * 2 + core

    right, left = lax.rem(h + 1, 4), lax.rem(h + 3, 4)
    partner = c + 1 - 2 * core

    chunk_ids = [lax.rem(h + 2, 4), right, left, h]
    loads = []
    k_load = pltpu.make_async_copy(k_hbm, kv.at[OWN, 0], load_sem.at[0])
    v_load = pltpu.make_async_copy(v_hbm, kv.at[OWN, 1], load_sem.at[1])
    k_load.start()
    v_load.start()
    for i, cid in enumerate(chunk_ids):
        src = q_hbm.at[pl.ds(pl.multiple_of(cid * chunk, chunk), chunk), :]
        cp = pltpu.make_async_copy(src, q_s.at[pl.ds(i * chunk, chunk), :], load_sem.at[2 + i])
        cp.start()
        loads.append(cp)
    w_load = pltpu.make_async_copy(w_hbm, w_s, w_sem)
    w_load.start()

    barrier = pltpu.get_barrier_semaphore()
    senders = [
        (at(-1, 0), h), (at(1, 0), h), (at(-2, 0), h), (at(3, 0), h),
        (at(0, -1), h), (at(0, 1), h), (partner, h), (c, left), (c, right),
    ]
    with scope("entry"):
        for dev in senders:
            pl.semaphore_signal(barrier, inc=1, device_id=dev, device_id_type=MESH)
        pl.semaphore_wait(barrier, len(senders))

    def kv_copy(src_slot, dst_slot, part, dev, sent_as=None):
        return pltpu.make_async_remote_copy(
            src_ref=kv.at[src_slot, part], dst_ref=kv.at[dst_slot, part],
            send_sem=kv_send.at[dst_slot if sent_as is None else sent_as, part],
            recv_sem=kv_recv.at[dst_slot, part],
            device_id=dev, device_id_type=MESH,
        )

    def arrived(slot, part):
        with scope(f"wait_{slot}_{part}"):
            kv_copy(OWN, slot, part, (c, h)).wait_recv()

    cut = rows * 3 // 4

    def cut_copy(src_slot, dst_slot, dev, low):
        part_rows = pl.ds(0, cut) if low else pl.ds(cut, rows - cut)
        sem = 0 if low else 1 if dst_slot == RELAY else 2
        return pltpu.make_async_remote_copy(
            src_ref=kv.at[src_slot, 0, part_rows], dst_ref=kv.at[dst_slot, 0, part_rows],
            send_sem=cut_send.at[sem], recv_sem=cut_recv.at[sem],
            device_id=dev, device_id_type=MESH,
        )

    z_up, z_up2, z_down, z_down3 = (at(1, 0), h), (at(2, 0), h), (at(-1, 0), h), (at(-3, 0), h)
    y_up, y_down = (at(0, 1), h), (at(0, -1), h)
    other = (partner, h)

    k_load.wait()
    v_load.wait()
    kv_copy(OWN, S8, 0, z_up).start()
    kv_copy(OWN, RELAY, 1, z_down).start()
    cut_copy(OWN, RELAY, z_down, False).start()
    kv_copy(OWN, S8, 1, z_up).start()

    @pl.when(y < 3)
    def _():
        kv_copy(OWN, S2, 0, y_up).start()
        kv_copy(OWN, S2, 1, y_up).start()

    @pl.when(core == 0)
    def _():
        kv_copy(OWN, S1, 0, other).start()
        kv_copy(OWN, S1, 1, other).start()

    scale = hd ** -0.5 * math.log2(math.e)
    blk_valid = valid_ref[c]
    ones_rows = vt.shape[1] - hd
    vt[:, hd:, :] = jnp.ones((vt.shape[0], ones_rows, rows), vt.dtype)
    acc[...] = jnp.zeros_like(acc)
    m_s[...] = jnp.full_like(m_s, -1e30)

    sub = rows // 2

    def tile_scores(slot, t, diag):
        pair, g = divmod(t, heads)
        q = q_s[pair * 2 * chunk:(pair + 1) * 2 * chunk, g * hd:(g + 1) * hd]
        m_old = m_s[t, 0:1, :]
        m_new = m_old
        for i in range(0, rows, sub):
            s = lax.dot_general(
                kv[slot, 0, i:i + sub, :], q, (((1,), (1,)), ((), ())), preferred_element_type=jnp.float32
            )
            if diag:
                key_at = i + lax.broadcasted_iota(jnp.int32, s.shape, 0)
                col = lax.broadcasted_iota(jnp.int32, s.shape, 1)
                first, second = chunk_ids[2 * pair], chunk_ids[2 * pair + 1]
                query_at = jnp.where(col < chunk, first * chunk + col, second * chunk + col - chunk)
                s = jnp.where((key_at <= query_at) & (key_at < blk_valid), s, -1e30)
            s_s[t % 2, i:i + sub] = s
            m_new = jnp.maximum(m_new, jnp.max(s, axis=0, keepdims=True))
        alpha_s[t % 3] = jnp.broadcast_to(jnp.exp2((m_old - m_new) * scale), alpha_s.shape[1:])
        m_s[t] = jnp.broadcast_to(m_new, m_s.shape[1:])

    def tile_weights(t):
        m = m_s[t, 0:1, :]
        for i in range(0, rows, sub):
            p_s[t % 2, i:i + sub] = jnp.exp2((s_s[t % 2, i:i + sub] - m) * scale).astype(p_s.dtype)

    def tile_mix(slot, t):
        pv = jnp.dot(vt[slot], p_s[t % 2], preferred_element_type=jnp.float32)
        acc[t] = acc[t] * alpha_s[t % 3, 0:1, :] + pv

    def tiles(slot, lo, hi, diag=False):
        tile_scores(slot, lo, diag)
        for t in range(lo, hi + 1):
            if t + 1 < hi:
                tile_scores(slot, t + 1, diag)
            if t < hi:
                tile_weights(t)
            if t > lo:
                tile_mix(slot, t - 1)

    def set_vt(slot):
        vt[slot, 0:hd, :] = kv[slot, 1].T

    def first_pair(slot):
        @pl.when(c >= OFFSETS[slot])
        def _():
            with scope(f"p0_{slot}"):
                set_vt(slot)
                tiles(slot, 0, heads)

    def second_pair(slot):
        @pl.when(c >= OFFSETS[slot])
        def _():
            with scope(f"p1_{slot}"):
                tiles(slot, heads, 2 * heads)

    with scope("blk_own"):
        for cp in loads:
            cp.wait()
        set_vt(OWN)
        tiles(OWN, 0, 2 * heads, True)

    @pl.when(core == 1)
    def _():
        arrived(S1, 0)
        arrived(S1, 1)
        first_pair(S1)

    def pass_on_s8(part):
        arrived(S8, part)
        kv_copy(S8, S16, part, z_up).start()

        @pl.when(y == 3)
        def _():
            kv_copy(S8, S2, part, y_up).start()

        @pl.when(y == 2)
        def _():
            kv_copy(S8, RELAY_Y, part, y_down).start()

    pass_on_s8(0)
    arrived(RELAY, 1)
    kv_copy(RELAY, S32, 1, z_down3).start()
    cut_copy(OWN, RELAY, (c, h), False).wait_recv()
    cut_copy(RELAY, S32, z_down3, False).start()

    @pl.when(core == 1)
    def _():
        second_pair(S1)

    pass_on_s8(1)

    def pass_on_s2(part):
        arrived(S2, part)

        @pl.when(core == 1)
        def _():
            kv_copy(S2, S1, part, other).start()

        @pl.when(y < 3)
        def _():
            kv_copy(S2, S4, part, y_up).start()

    @pl.when(y > 0)
    def _():
        pass_on_s2(0)
        pass_on_s2(1)

    @pl.when(c >= OFFSETS[S8])
    def _():
        with scope("both_s8"):
            set_vt(S8)
            tiles(S8, 0, 2 * heads)

    @pl.when(y > 0)
    def _():
        first_pair(S2)

    arrived(S16, 0)
    cut_copy(S16, S32, z_up2, True).start()

    def relay_y(part):
        @pl.when(y == 1)
        def _():
            arrived(RELAY_Y, part)
            kv_copy(RELAY_Y, S4, part, y_down, sent_as=RELAY_Y).start()

    def first_s1():
        arrived(S1, 0)
        arrived(S1, 1)
        first_pair(S1)

    relay_y(0)

    @pl.when(y == 0)
    def _():
        pass_on_s2(0)

    pl.when((core == 0) & (y > 0))(first_s1)
    arrived(S16, 1)
    relay_y(1)
    first_pair(S16)

    @pl.when(y == 0)
    def _():
        pass_on_s2(1)
        first_pair(S2)

    pl.when((core == 0) & (y == 0))(first_s1)
    early = (core == 1) & (y > 0)

    @pl.when(early)
    def _():
        second_pair(S2)

    def first_s4():
        arrived(S4, 0)
        arrived(S4, 1)
        first_pair(S4)

    pl.when(y != 1)(first_s4)
    cut_copy(OWN, S32, (c, h), True).wait_recv()
    cut_copy(OWN, S32, (c, h), False).wait_recv()
    arrived(S32, 1)
    first_pair(S32)
    pl.when(y == 1)(first_s4)

    def finish(pair):
        for g in range(heads):
            full = acc[pair * heads + g]
            mix = full[:hd, :] / full[hd:hd + 1, :]
            att[pair * 2 * chunk:(pair + 1) * 2 * chunk, g * hd:(g + 1) * hd] = mix.T.astype(jnp.bfloat16)

    def partial(i, piece):
        cols = pl.ds(piece * pw if isinstance(piece, int) else pl.multiple_of(piece * pw, pw), pw)
        return jnp.dot(
            att[i * chunk:(i + 1) * chunk, :], w_s[:, cols], preferred_element_type=jnp.float32
        )

    def far_copy(side, j):
        piece = j if side == 0 else half + j
        return pltpu.make_async_remote_copy(
            src_ref=far_send.at[piece], dst_ref=far_recv.at[side, j],
            send_sem=fs_sem.at[side, j], recv_sem=fr_sem.at[side, j],
            device_id=(c, right if side == 0 else left), device_id_type=MESH,
        )

    def near_copy(side, piece):
        return pltpu.make_async_remote_copy(
            src_ref=near_send.at[side, piece], dst_ref=near_recv.at[side, piece],
            send_sem=ns_sem.at[side, piece], recv_sem=nr_sem.at[side, piece],
            device_id=(c, right if side == 0 else left), device_id_type=MESH,
        )

    with scope("finish_0"):
        finish(0)
        w_load.wait()

    bf16 = jnp.bfloat16

    with scope("far"):

        @pl.loop(0, half)
        def _(j):
            low, high = partial(0, j), partial(0, half + j)
            far_send[j] = low.astype(bf16)
            far_send[half + j] = high.astype(bf16)
            far_copy(0, j).start()
            far_copy(1, j).start()

    def plain(side, pieces):
        for at_piece in range(0, len(pieces), 2):
            group = pieces[at_piece:at_piece + 2]
            parts = [partial(1 + side, piece) for piece in group]
            for piece, value in zip(group, parts):
                near_send[side, piece] = value.astype(bf16)
            for piece in group:
                near_copy(side, piece).start()

    with scope("plain_right"):
        plain(0, list(range(half, np_)))

    @pl.when(jnp.logical_not(early))
    def _():
        second_pair(S2)

    @pl.when(core == 0)
    def _():
        second_pair(S1)

    for slot in (S16, S4, S32):
        second_pair(slot)

    with scope("finish_1"):
        finish(1)

    with scope("plain_left"):
        plain(1, list(range(half)))

    with scope("near_sum"):

        @pl.loop(0, half)
        def _(j):
            low, high = partial(1, j), partial(2, half + j)
            far_copy(0, j).wait_recv()
            near_send[0, j] = (low + far_recv[0, j].astype(jnp.float32)).astype(bf16)
            near_copy(0, j).start()
            far_copy(1, j).wait_recv()
            near_send[1, half + j] = (high + far_recv[1, j].astype(jnp.float32)).astype(bf16)
            near_copy(1, half + j).start()

    with scope("own_part"):

        @pl.loop(0, half)
        def _(j):
            low, high = partial(3, j), partial(3, half + j)
            own_s[j] = low
            own_s[half + j] = high

    def final(piece):
        near_copy(0, piece).wait_recv()
        near_copy(1, piece).wait_recv()
        o_ref[:, pl.ds(pl.multiple_of(piece * pw, pw), pw)] = (
            own_s[piece] + near_recv[0, piece].astype(jnp.float32) + near_recv[1, piece].astype(jnp.float32)
        ).astype(o_ref.dtype)

    with scope("final"):
        @pl.loop(0, half)
        def _(j):
            final(j)
            final(half + j)

    for part in range(2):
        for slot in (S2, S1, S8, S16):
            kv_copy(OWN, slot, part, (c, h)).wait_send()

        @pl.when(y < 3)
        def _():
            kv_copy(OWN, S4, part, (c, h)).wait_send()

        @pl.when((y == 1) | (y == 2))
        def _():
            kv_copy(OWN, RELAY_Y, part, (c, h)).wait_send()
    kv_copy(OWN, RELAY, 1, (c, h)).wait_send()
    kv_copy(OWN, S32, 1, (c, h)).wait_send()
    cut_copy(OWN, S32, (c, h), True).wait_send()
    cut_copy(OWN, RELAY, (c, h), False).wait_send()
    cut_copy(OWN, S32, (c, h), False).wait_send()

    @pl.loop(0, half)
    def _(j):
        far_copy(0, j).wait_send()
        far_copy(1, j).wait_send()

    @pl.loop(0, np_)
    def _(j):
        near_copy(0, j).wait_send()
        near_copy(1, j).wait_send()


def per_device(queries, key_block, value_block, block_valid, out_weight):
    rows, qcols = queries.shape
    hd = key_block.shape[1]
    heads = qcols // hd
    d = out_weight.shape[1]
    chunk = rows // 4
    pw = 256
    np_ = d // pw
    half = np_ // 2
    bf16, f32 = jnp.bfloat16, jnp.float32
    any_spec = pl.BlockSpec(memory_space=pl.ANY)
    return pl.pallas_call(
        kernel,
        out_shape=pltpu.VMEM((chunk, d), bf16),
        in_specs=[pl.BlockSpec(memory_space=pltpu.SMEM)] + [any_spec] * 4,
        out_specs=pl.BlockSpec(memory_space=pltpu.VMEM),
        scratch_shapes=[
            pltpu.VMEM((rows, qcols), bf16),
            pltpu.VMEM((9, 2, rows, hd), bf16),
            pltpu.VMEM((7, hd + 16, rows), bf16),
            pltpu.VMEM((qcols, d), bf16),
            pltpu.VMEM((2 * heads, hd + 16, 2 * chunk), f32),
            pltpu.VMEM((2 * heads, 8, 2 * chunk), f32),
            pltpu.VMEM((2, rows, 2 * chunk), f32),
            pltpu.VMEM((2, rows, 2 * chunk), bf16),
            pltpu.VMEM((3, 8, 2 * chunk), f32),
            pltpu.VMEM((rows, qcols), bf16),
            pltpu.VMEM((np_, chunk, pw), f32),
            pltpu.VMEM((np_, chunk, pw), bf16),
            pltpu.VMEM((2, half, chunk, pw), bf16),
            pltpu.VMEM((2, np_, chunk, pw), bf16),
            pltpu.VMEM((2, np_, chunk, pw), bf16),
            pltpu.SemaphoreType.DMA((6,)),
            pltpu.SemaphoreType.DMA,
            pltpu.SemaphoreType.DMA((9, 2)),
            pltpu.SemaphoreType.DMA((9, 2)),
            pltpu.SemaphoreType.DMA((3,)),
            pltpu.SemaphoreType.DMA((3,)),
            pltpu.SemaphoreType.DMA((2, half)),
            pltpu.SemaphoreType.DMA((2, half)),
            pltpu.SemaphoreType.DMA((2, np_)),
            pltpu.SemaphoreType.DMA((2, np_)),
        ],
        compiler_params=pltpu.CompilerParams(
            collective_id=0, has_side_effects=True, vmem_limit_bytes=65_900_000
        ),
        name="attend_project",
    )(block_valid, queries, key_block, value_block, out_weight)


def solution(mesh):
    return jax.shard_map(
        per_device,
        mesh=mesh,
        in_specs=(P("ctx", "kvh"), P("ctx", "kvh"), P("ctx", "kvh"), P(), P("kvh", None)),
        out_specs=P(("ctx", "kvh"), None),
        check_vma=False,
    )
```

```python
import contextlib
import math

import jax
import jax.numpy as jnp
from jax import lax
from jax.experimental import pallas as pl
from jax.experimental.pallas import tpu as pltpu
from jax.sharding import PartitionSpec as P

MESH = pl.DeviceIdType.MESH
TRACE = False
OWN, S1, S2, S4, S8, S16, S32, RELAY, RELAY_Y = range(9)
OFFSETS = {S1: 1, S2: 2, S4: 4, S8: 8, S16: 16, S32: 32}


def scope(name):
    return jax.named_scope(name) if TRACE else contextlib.nullcontext()


def kernel(
    valid_ref, q_hbm, k_hbm, v_hbm, w_hbm, o_ref,
    q_s, kv, vt, w_s, acc, m_s, s_s, p_s, alpha_s, att, own_s,
    far_send, far_recv, near_send, near_recv,
    load_sem, w_sem, kv_send, kv_recv, cut_send, cut_recv, fs_sem, fr_sem, ns_sem, nr_sem,
):
    rows, qcols = q_hbm.shape
    hd = k_hbm.shape[1]
    heads = qcols // hd
    chunk = rows // 4
    pw = own_s.shape[2]
    np_ = own_s.shape[0]
    half = np_ // 2
    c = lax.axis_index("ctx")
    h = lax.axis_index("kvh")
    core = lax.rem(c, 2)
    y = lax.rem(c // 2, 4)
    z = c // 8

    def at(dz, dy):
        return lax.rem(z + 8 + dz, 8) * 8 + lax.rem(y + 4 + dy, 4) * 2 + core

    right, left = lax.rem(h + 1, 4), lax.rem(h + 3, 4)
    partner = c + 1 - 2 * core

    chunk_ids = [lax.rem(h + 2, 4), right, left, h]
    loads = []
    k_load = pltpu.make_async_copy(k_hbm, kv.at[OWN, 0], load_sem.at[0])
    v_load = pltpu.make_async_copy(v_hbm, kv.at[OWN, 1], load_sem.at[1])
    k_load.start()
    v_load.start()
    for i, cid in enumerate(chunk_ids):
        src = q_hbm.at[pl.ds(pl.multiple_of(cid * chunk, chunk), chunk), :]
        cp = pltpu.make_async_copy(src, q_s.at[pl.ds(i * chunk, chunk), :], load_sem.at[2 + i])
        cp.start()
        loads.append(cp)
    w_load = pltpu.make_async_copy(w_hbm, w_s, w_sem)
    w_load.start()

    barrier = pltpu.get_barrier_semaphore()
    senders = [
        (at(-1, 0), h), (at(1, 0), h), (at(-2, 0), h), (at(3, 0), h),
        (at(0, -1), h), (at(0, 1), h), (partner, h), (c, left), (c, right),
    ]
    with scope("entry"):
        for dev in senders:
            pl.semaphore_signal(barrier, inc=1, device_id=dev, device_id_type=MESH)
        pl.semaphore_wait(barrier, len(senders))

    def kv_copy(src_slot, dst_slot, part, dev, sent_as=None):
        return pltpu.make_async_remote_copy(
            src_ref=kv.at[src_slot, part], dst_ref=kv.at[dst_slot, part],
            send_sem=kv_send.at[dst_slot if sent_as is None else sent_as, part],
            recv_sem=kv_recv.at[dst_slot, part],
            device_id=dev, device_id_type=MESH,
        )

    def arrived(slot, part):
        with scope(f"wait_{slot}_{part}"):
            kv_copy(OWN, slot, part, (c, h)).wait_recv()

    cut = rows * 3 // 4

    def cut_copy(src_slot, dst_slot, dev, low):
        part_rows = pl.ds(0, cut) if low else pl.ds(cut, rows - cut)
        sem = 0 if low else 1 if dst_slot == RELAY else 2
        return pltpu.make_async_remote_copy(
            src_ref=kv.at[src_slot, 0, part_rows], dst_ref=kv.at[dst_slot, 0, part_rows],
            send_sem=cut_send.at[sem], recv_sem=cut_recv.at[sem],
            device_id=dev, device_id_type=MESH,
        )

    z_up, z_up2, z_down, z_down3 = (at(1, 0), h), (at(2, 0), h), (at(-1, 0), h), (at(-3, 0), h)
    y_up, y_down = (at(0, 1), h), (at(0, -1), h)
    other = (partner, h)

    k_load.wait()
    v_load.wait()
    kv_copy(OWN, S8, 0, z_up).start()
    kv_copy(OWN, RELAY, 1, z_down).start()
    cut_copy(OWN, RELAY, z_down, False).start()
    kv_copy(OWN, S8, 1, z_up).start()

    @pl.when(y < 3)
    def _():
        kv_copy(OWN, S2, 0, y_up).start()
        kv_copy(OWN, S2, 1, y_up).start()

    @pl.when(core == 0)
    def _():
        kv_copy(OWN, S1, 0, other).start()
        kv_copy(OWN, S1, 1, other).start()

    scale = hd ** -0.5 * math.log2(math.e)
    blk_valid = valid_ref[c]
    ones_rows = vt.shape[1] - hd
    vt[:, hd:, :] = jnp.ones((vt.shape[0], ones_rows, rows), vt.dtype)
    acc[...] = jnp.zeros_like(acc)
    m_s[...] = jnp.full_like(m_s, -1e30)

    sub = rows // 2

    def tile_scores(slot, t, diag):
        pair, g = divmod(t, heads)
        q = q_s[pair * 2 * chunk:(pair + 1) * 2 * chunk, g * hd:(g + 1) * hd]
        m_old = m_s[t, 0:1, :]
        m_new = m_old
        for i in range(0, rows, sub):
            s = lax.dot_general(
                kv[slot, 0, i:i + sub, :], q, (((1,), (1,)), ((), ())), preferred_element_type=jnp.float32
            )
            if diag:
                key_at = i + lax.broadcasted_iota(jnp.int32, s.shape, 0)
                col = lax.broadcasted_iota(jnp.int32, s.shape, 1)
                first, second = chunk_ids[2 * pair], chunk_ids[2 * pair + 1]
                query_at = jnp.where(col < chunk, first * chunk + col, second * chunk + col - chunk)
                s = jnp.where((key_at <= query_at) & (key_at < blk_valid), s, -1e30)
            s_s[t % 2, i:i + sub] = s
            m_new = jnp.maximum(m_new, jnp.max(s, axis=0, keepdims=True))
        alpha_s[t % 3] = jnp.broadcast_to(jnp.exp2((m_old - m_new) * scale), alpha_s.shape[1:])
        m_s[t] = jnp.broadcast_to(m_new, m_s.shape[1:])

    def tile_weights(t):
        m = m_s[t, 0:1, :]
        for i in range(0, rows, sub):
            p_s[t % 2, i:i + sub] = jnp.exp2((s_s[t % 2, i:i + sub] - m) * scale).astype(p_s.dtype)

    def tile_mix(slot, t):
        pv = jnp.dot(vt[slot], p_s[t % 2], preferred_element_type=jnp.float32)
        acc[t] = acc[t] * alpha_s[t % 3, 0:1, :] + pv

    def tiles(slot, lo, hi, diag=False):
        tile_scores(slot, lo, diag)
        for t in range(lo, hi + 1):
            if t + 1 < hi:
                tile_scores(slot, t + 1, diag)
            if t < hi:
                tile_weights(t)
            if t > lo:
                tile_mix(slot, t - 1)

    def set_vt(slot):
        vt[slot, 0:hd, :] = kv[slot, 1].T

    def first_pair(slot):
        @pl.when(c >= OFFSETS[slot])
        def _():
            with scope(f"p0_{slot}"):
                set_vt(slot)
                tiles(slot, 0, heads)

    def second_pair(slot):
        @pl.when(c >= OFFSETS[slot])
        def _():
            with scope(f"p1_{slot}"):
                tiles(slot, heads, 2 * heads)

    with scope("blk_own"):
        for cp in loads:
            cp.wait()
        set_vt(OWN)
        tiles(OWN, 0, 2 * heads, True)

    @pl.when(core == 1)
    def _():
        arrived(S1, 0)
        arrived(S1, 1)
        first_pair(S1)

    def pass_on_s8(part):
        arrived(S8, part)
        kv_copy(S8, S16, part, z_up).start()

        @pl.when(y == 3)
        def _():
            kv_copy(S8, S2, part, y_up).start()

        @pl.when(y == 2)
        def _():
            kv_copy(S8, RELAY_Y, part, y_down).start()

    pass_on_s8(0)
    arrived(RELAY, 1)
    kv_copy(RELAY, S32, 1, z_down3).start()
    cut_copy(OWN, RELAY, (c, h), False).wait_recv()
    cut_copy(RELAY, S32, z_down3, False).start()

    @pl.when(core == 1)
    def _():
        second_pair(S1)

    pass_on_s8(1)

    def pass_on_s2(part):
        arrived(S2, part)

        @pl.when(core == 1)
        def _():
            kv_copy(S2, S1, part, other).start()

        @pl.when(y < 3)
        def _():
            kv_copy(S2, S4, part, y_up).start()

    @pl.when(y > 0)
    def _():
        pass_on_s2(0)
        pass_on_s2(1)

    @pl.when(c >= OFFSETS[S8])
    def _():
        with scope("both_s8"):
            set_vt(S8)
            tiles(S8, 0, 2 * heads)

    @pl.when(y > 0)
    def _():
        first_pair(S2)

    arrived(S16, 0)
    cut_copy(S16, S32, z_up2, True).start()

    def relay_y(part):
        @pl.when(y == 1)
        def _():
            arrived(RELAY_Y, part)
            kv_copy(RELAY_Y, S4, part, y_down, sent_as=RELAY_Y).start()

    def first_s1():
        arrived(S1, 0)
        arrived(S1, 1)
        first_pair(S1)

    relay_y(0)

    @pl.when(y == 0)
    def _():
        pass_on_s2(0)

    pl.when((core == 0) & (y > 0))(first_s1)

    @pl.when(c >= OFFSETS[S16])
    def _():
        arrived(S16, 1)

    relay_y(1)
    first_pair(S16)

    @pl.when(y == 0)
    def _():
        pass_on_s2(1)
        first_pair(S2)

    pl.when((core == 0) & (y == 0))(first_s1)
    early = (core == 1) & (y > 0)

    @pl.when(early)
    def _():
        second_pair(S2)

    def first_s4():
        arrived(S4, 0)
        arrived(S4, 1)
        first_pair(S4)

    def wait_s32():
        cut_copy(OWN, S32, (c, h), True).wait_recv()
        cut_copy(OWN, S32, (c, h), False).wait_recv()
        arrived(S32, 1)

    pl.when(y > 1)(first_s4)
    pl.when(c >= OFFSETS[S32])(wait_s32)
    first_pair(S32)
    pl.when(y <= 1)(first_s4)

    def finish(pair):
        for g in range(heads):
            full = acc[pair * heads + g]
            mix = full[:hd, :] / full[hd:hd + 1, :]
            att[pair * 2 * chunk:(pair + 1) * 2 * chunk, g * hd:(g + 1) * hd] = mix.T.astype(jnp.bfloat16)

    def partial(i, piece):
        cols = pl.ds(piece * pw if isinstance(piece, int) else pl.multiple_of(piece * pw, pw), pw)
        return jnp.dot(
            att[i * chunk:(i + 1) * chunk, :], w_s[:, cols], preferred_element_type=jnp.float32
        )

    def far_copy(side, j):
        piece = j if side == 0 else half + j
        return pltpu.make_async_remote_copy(
            src_ref=far_send.at[piece], dst_ref=far_recv.at[side, j],
            send_sem=fs_sem.at[side, j], recv_sem=fr_sem.at[side, j],
            device_id=(c, right if side == 0 else left), device_id_type=MESH,
        )

    def near_copy(side, piece):
        return pltpu.make_async_remote_copy(
            src_ref=near_send.at[side, piece], dst_ref=near_recv.at[side, piece],
            send_sem=ns_sem.at[side, piece], recv_sem=nr_sem.at[side, piece],
            device_id=(c, right if side == 0 else left), device_id_type=MESH,
        )

    with scope("finish_0"):
        finish(0)
        w_load.wait()

    bf16 = jnp.bfloat16

    with scope("far"):

        @pl.loop(0, half)
        def _(j):
            low, high = partial(0, j), partial(0, half + j)
            far_send[j] = low.astype(bf16)
            far_send[half + j] = high.astype(bf16)
            far_copy(0, j).start()
            far_copy(1, j).start()

    def plain(side, pieces):
        for at_piece in range(0, len(pieces), 2):
            group = pieces[at_piece:at_piece + 2]
            parts = [partial(1 + side, piece) for piece in group]
            for piece, value in zip(group, parts):
                near_send[side, piece] = value.astype(bf16)
            for piece in group:
                near_copy(side, piece).start()

    with scope("plain_right"):
        plain(0, list(range(half, np_)))

    @pl.when(jnp.logical_not(early))
    def _():
        second_pair(S2)

    @pl.when(core == 0)
    def _():
        second_pair(S1)

    for slot in (S16, S4, S32):
        second_pair(slot)

    with scope("finish_1"):
        finish(1)

    with scope("plain_left"):
        plain(1, list(range(half)))

    with scope("near_sum"):

        @pl.loop(0, half)
        def _(j):
            low, high = partial(1, j), partial(2, half + j)
            far_copy(0, j).wait_recv()
            near_send[0, j] = (low + far_recv[0, j].astype(jnp.float32)).astype(bf16)
            near_copy(0, j).start()
            far_copy(1, j).wait_recv()
            near_send[1, half + j] = (high + far_recv[1, j].astype(jnp.float32)).astype(bf16)
            near_copy(1, half + j).start()

    with scope("own_part"):

        @pl.loop(0, half)
        def _(j):
            low, high = partial(3, j), partial(3, half + j)
            own_s[j] = low
            own_s[half + j] = high

    def final(piece):
        near_copy(0, piece).wait_recv()
        near_copy(1, piece).wait_recv()
        o_ref[:, pl.ds(pl.multiple_of(piece * pw, pw), pw)] = (
            own_s[piece] + near_recv[0, piece].astype(jnp.float32) + near_recv[1, piece].astype(jnp.float32)
        ).astype(o_ref.dtype)

    with scope("final"):
        @pl.loop(0, half)
        def _(j):
            final(j)
            final(half + j)

    pl.when(c < OFFSETS[S32])(wait_s32)

    @pl.when(c < OFFSETS[S16])
    def _():
        arrived(S16, 1)

    for part in range(2):
        for slot in (S2, S1, S8, S16):
            kv_copy(OWN, slot, part, (c, h)).wait_send()

        @pl.when(y < 3)
        def _():
            kv_copy(OWN, S4, part, (c, h)).wait_send()

        @pl.when((y == 1) | (y == 2))
        def _():
            kv_copy(OWN, RELAY_Y, part, (c, h)).wait_send()
    kv_copy(OWN, RELAY, 1, (c, h)).wait_send()
    kv_copy(OWN, S32, 1, (c, h)).wait_send()
    cut_copy(OWN, S32, (c, h), True).wait_send()
    cut_copy(OWN, RELAY, (c, h), False).wait_send()
    cut_copy(OWN, S32, (c, h), False).wait_send()

    @pl.loop(0, half)
    def _(j):
        far_copy(0, j).wait_send()
        far_copy(1, j).wait_send()

    @pl.loop(0, np_)
    def _(j):
        near_copy(0, j).wait_send()
        near_copy(1, j).wait_send()


def per_device(queries, key_block, value_block, block_valid, out_weight):
    rows, qcols = queries.shape
    hd = key_block.shape[1]
    heads = qcols // hd
    d = out_weight.shape[1]
    chunk = rows // 4
    pw = 256
    np_ = d // pw
    half = np_ // 2
    bf16, f32 = jnp.bfloat16, jnp.float32
    any_spec = pl.BlockSpec(memory_space=pl.ANY)
    return pl.pallas_call(
        kernel,
        out_shape=pltpu.VMEM((chunk, d), bf16),
        in_specs=[pl.BlockSpec(memory_space=pltpu.SMEM)] + [any_spec] * 4,
        out_specs=pl.BlockSpec(memory_space=pltpu.VMEM),
        scratch_shapes=[
            pltpu.VMEM((rows, qcols), bf16),
            pltpu.VMEM((9, 2, rows, hd), bf16),
            pltpu.VMEM((7, hd + 16, rows), bf16),
            pltpu.VMEM((qcols, d), bf16),
            pltpu.VMEM((2 * heads, hd + 16, 2 * chunk), f32),
            pltpu.VMEM((2 * heads, 8, 2 * chunk), f32),
            pltpu.VMEM((2, rows, 2 * chunk), f32),
            pltpu.VMEM((2, rows, 2 * chunk), bf16),
            pltpu.VMEM((3, 8, 2 * chunk), f32),
            pltpu.VMEM((rows, qcols), bf16),
            pltpu.VMEM((np_, chunk, pw), f32),
            pltpu.VMEM((np_, chunk, pw), bf16),
            pltpu.VMEM((2, half, chunk, pw), bf16),
            pltpu.VMEM((2, np_, chunk, pw), bf16),
            pltpu.VMEM((2, np_, chunk, pw), bf16),
            pltpu.SemaphoreType.DMA((6,)),
            pltpu.SemaphoreType.DMA,
            pltpu.SemaphoreType.DMA((9, 2)),
            pltpu.SemaphoreType.DMA((9, 2)),
            pltpu.SemaphoreType.DMA((3,)),
            pltpu.SemaphoreType.DMA((3,)),
            pltpu.SemaphoreType.DMA((2, half)),
            pltpu.SemaphoreType.DMA((2, half)),
            pltpu.SemaphoreType.DMA((2, np_)),
            pltpu.SemaphoreType.DMA((2, np_)),
        ],
        compiler_params=pltpu.CompilerParams(
            collective_id=0, has_side_effects=True, vmem_limit_bytes=65_900_000
        ),
        name="attend_project",
    )(block_valid, queries, key_block, value_block, out_weight)


def solution(mesh):
    return jax.shard_map(
        per_device,
        mesh=mesh,
        in_specs=(P("ctx", "kvh"), P("ctx", "kvh"), P("ctx", "kvh"), P(), P("kvh", None)),
        out_specs=P(("ctx", "kvh"), None),
        check_vma=False,
    )
```
